32 devices in a mesh: rows: 16 (over z, y, x), cols: 2 (over core).
Axes of the slice: x: 2, y: 2, z: 4, core: 2. Of those that a mesh axis runs over, the one named last changes fastest.
Arguments:
- design: float32 [16384, 512], P('rows', 'cols'), may hold values from -24 to 24
- signs: int32 [16384], P('rows'), may hold values from -1 to 1, as said below
- kept: int32 [1024], replicated, may hold values from 0 to 16383, as said below
Outputs:
- sketch: float32 [1024, 512], P('rows', 'cols')
- factor: float32 [512, 512], P(None, 'cols')
The draws below stay inside these ranges and needn't reach their ends.
Inputs may be any that keep to these rules, and one draw needn't show every extreme that they name: `signs`: each entry is +1 or -1. `kept`: distinct and increasing.
All inputs are finite; a program needn't handle non-finite values.
Results may differ from the reference program's by a relative error of at most 0.0003.
Values sent between devices are 32-bit elements; how exact they have to be, the bound alone decides.
A program may use at most 64 MiB of HBM per device.

```python
import math
import jax
import jax.numpy as jnp
from jax import lax

P_SIZE = 512
ROWS_DEV = 1024
ROWS = 16384
KEPT = 1024
N_ROWS = 16


def draw_design(key, part):
    base = jax.random.fold_in(key, 11)
    first, second, third = jax.random.split(base, 3)
    column_scales = jnp.exp(jax.random.uniform(first, (P_SIZE,), jnp.float32, jnp.log(0.3), jnp.log(3.0)))
    noise = jax.random.normal(second, (ROWS, P_SIZE), jnp.float32)
    common = jax.random.normal(third, (ROWS, 1), jnp.float32)
    values = (noise + 0.6 * common) * column_scales[None, :]
    return jnp.clip(values, -24.0, 24.0).astype(jnp.float32)


def draw_signs(key, part):
    base = jax.random.fold_in(key, 22)
    return (2 * jax.random.randint(base, (ROWS,), 0, 2) - 1).astype(jnp.int32)


def draw_kept(key, part):
    base = jax.random.fold_in(key, 33)
    chosen = jax.random.permutation(base, ROWS)[:KEPT]
    return jnp.sort(chosen).astype(jnp.int32)


def setup_inputs(seed: int = 0) -> dict:
    arg_keys = jax.random.split(jax.random.key(seed), 4)
    design = draw_design(jax.random.fold_in(arg_keys[3], 71), 0)
    signs = draw_signs(jax.random.fold_in(arg_keys[3], 71), 0)
    kept = draw_kept(jax.random.fold_in(arg_keys[3], 71), 0)
    return dict(design=design, signs=signs, kept=kept)


def hadamard(order):
    matrix = jnp.ones((1, 1), jnp.float32)
    base = jnp.array([[1.0, 1.0], [1.0, -1.0]], jnp.float32)
    while matrix.shape[0] < order:
        matrix = jnp.kron(matrix, base)
    return matrix

def bit_parity(value):
    folded = value.astype(jnp.int32)
    for amount in (16, 8, 4, 2, 1):
        folded = jnp.bitwise_xor(folded, jnp.right_shift(folded, amount))
    return jnp.bitwise_and(folded, 1)

def local_transform(flipped):
    length, width = flipped.shape
    outer = length // 128
    inner_table = hadamard(128)
    outer_table = hadamard(outer)
    blocks = flipped.reshape(outer, 128, width)
    mixed = jnp.einsum('pb,abc->apc', inner_table, blocks, precision=lax.Precision.HIGHEST)
    mixed = jnp.einsum('qa,apc->qpc', outer_table, mixed, precision=lax.Precision.HIGHEST)
    return mixed.reshape(length, width)

def reference(design, signs, kept):
    length = ROWS_DEV
    kept_blocks = (kept // length).astype(jnp.int32)
    offsets = (kept - kept_blocks * length).astype(jnp.int32)
    scale = 1.0 / math.sqrt(ROWS)

    def step(total, block_row):
        start = (block_row * length).astype(jnp.int32)
        piece = lax.dynamic_slice_in_dim(design, start, length, 0)
        flips = lax.dynamic_slice_in_dim(signs, start, length, 0)
        transformed = local_transform(piece * flips.astype(jnp.float32)[:, None])
        parity = bit_parity(jnp.bitwise_and(kept_blocks, block_row))
        factor = (1.0 - 2.0 * parity.astype(jnp.float32)) * scale
        return (total + jnp.take(transformed, offsets, axis=0) * factor[:, None], None)
    start_total = jnp.zeros((KEPT, P_SIZE), jnp.float32)
    sketch, unused = lax.scan(step, start_total, jnp.arange(N_ROWS, dtype=jnp.int32))
    gram = jnp.dot(sketch.T.astype(jnp.float32), sketch.astype(jnp.float32), precision=lax.Precision.HIGHEST, preferred_element_type=jnp.float32) / KEPT
    factor = jnp.linalg.cholesky(gram).T
    return (sketch, factor)
```

```python
import functools
import math

import jax
import jax.numpy as jnp
from jax import lax
from jax.experimental import pallas as pl
from jax.experimental.pallas import tpu as pltpu
from jax.sharding import PartitionSpec as P

MESH = pl.DeviceIdType.MESH
HIGHEST = lax.Precision.HIGHEST
LANES = 128


def transform_kernel(scale, tile, design_ref, signs_ref, kept_ref, out_ref, split):
    length = design_ref.shape[0]
    values = design_ref[...]
    high = values.astype(jnp.bfloat16)
    rest = values - high.astype(jnp.float32)
    middle = rest.astype(jnp.bfloat16)
    split[0] = high
    split[1] = middle
    split[2] = (rest - middle.astype(jnp.float32)).astype(jnp.bfloat16)
    first_row = lax.axis_index("rows") * length
    lane = lax.broadcasted_iota(jnp.int32, (LANES, LANES), 1)

    def step(index, carry):
        stacked = []
        for piece in range(tile // LANES):
            row = kept_ref[pl.ds(index * (tile // LANES) + piece, 1), :]
            column = jnp.broadcast_to(row, (LANES, LANES)).T
            blocks = []
            for block in range(length // LANES):
                common = jnp.bitwise_and(column, lane + (first_row + block * LANES))
                odd = jnp.bitwise_and(lax.population_count(common), 1)
                flips = signs_ref[block : block + 1, :]
                entry = (1 - 2 * odd) * flips
                blocks.append(entry.astype(jnp.float32).astype(jnp.bfloat16))
            stacked.append(jnp.concatenate(blocks, axis=1))
        table = jnp.concatenate(stacked, axis=0)
        total = jnp.dot(table, split[2], preferred_element_type=jnp.float32)
        total += jnp.dot(table, split[1], preferred_element_type=jnp.float32)
        total += jnp.dot(table, split[0], preferred_element_type=jnp.float32)
        out_ref[pl.ds(pl.multiple_of(index * tile, tile), tile), :] = total * scale
        return carry

    lax.fori_loop(0, out_ref.shape[0] // tile, step, 0)


def transform(design, signs, kept, total_rows):
    length, width = design.shape
    count = kept.shape[0]
    tile = 256
    return pl.pallas_call(
        functools.partial(transform_kernel, 1.0 / math.sqrt(total_rows), tile),
        out_shape=jax.ShapeDtypeStruct((count, width), jnp.float32),
        in_specs=[pl.BlockSpec(memory_space=pltpu.VMEM)] * 3,
        out_specs=pl.BlockSpec(memory_space=pltpu.VMEM),
        scratch_shapes=[pltpu.VMEM((3, length, width), jnp.bfloat16)],
        cost_estimate=pl.CostEstimate(
            flops=6 * count * length * width, bytes_accessed=4 * (count + length) * width, transcendentals=0
        ),
    )(design, signs.reshape(-1, LANES), kept.reshape(-1, LANES))


def exchange_kernel(
    n, orders, x_ref, sketch_ref, gram_ref, buf, recv, gat,
    rs_send, rs_recv, ag_send, ag_recv, ex_send, ex_recv,
):
    me = lax.axis_index("rows")
    core = lax.axis_index("cols")
    levels = len(orders[0])
    parts = len(orders)
    width = x_ref.shape[2]
    sub = x_ref.shape[1] // parts

    def flip(bit):
        return (1 - 2 * ((me // (1 << bit)) % 2)) * (1 << bit)

    barrier = pltpu.get_barrier_semaphore()
    for bit in range(levels):
        pl.semaphore_signal(barrier, inc=1, device_id=(me + flip(bit), core), device_id_type=MESH)
    pl.semaphore_signal(barrier, inc=1, device_id=(me, 1 - core), device_id_type=MESH)

    def slot_owner(part, slot):
        owner = me
        for place, bit in enumerate(orders[part]):
            if (slot >> (levels - 1 - place)) & 1:
                owner = owner + flip(bit)
        return owner

    lanes = pl.ds(pl.multiple_of(core * width, LANES), width)

    for part in range(parts):
        for slot in range(n - 1, -1, -1):
            buf[part, slot] = x_ref[slot_owner(part, slot), part * sub : (part + 1) * sub, :]
    pl.semaphore_wait(barrier, levels + 1)

    def reduce_copy(part, level):
        half = n >> (level + 1)
        return pltpu.make_async_remote_copy(
            src_ref=buf.at[part, pl.ds(half, half)],
            dst_ref=recv.at[part, pl.ds(half, half)],
            send_sem=rs_send.at[part, level],
            recv_sem=rs_recv.at[part, level],
            device_id=(me + flip(orders[part][level]), core),
            device_id_type=MESH,
        )

    for part in range(parts):
        reduce_copy(part, 0).start()
    for level in range(levels):
        half = n >> (level + 1)
        for part in range(parts):
            reduce_copy(part, level).wait_recv()
            if level + 1 < levels:
                low = half // 2
                buf[part, low:half] += recv[part, half + low : 2 * half]
                reduce_copy(part, level + 1).start()
                buf[part, 0:low] += recv[part, half : half + low]
            else:
                own = buf[part, 0] + recv[part, 1]
                sketch_ref[part * sub : (part + 1) * sub, :] = own
                gat[part, 0, :, lanes] = own

    def gather_copy(part, level):
        half = n >> (level + 1)
        return pltpu.make_async_remote_copy(
            src_ref=gat.at[part, pl.ds(0, half), :, lanes],
            dst_ref=gat.at[part, pl.ds(half, half), :, lanes],
            send_sem=ag_send.at[part, level],
            recv_sem=ag_recv.at[part, level],
            device_id=(me + flip(orders[part][level]), core),
            device_id_type=MESH,
        )

    def core_copy(part, level):
        start, size = (0, 1) if level == levels else (n >> (level + 1), n >> (level + 1))
        return pltpu.make_async_remote_copy(
            src_ref=gat.at[part, pl.ds(start, size), :, lanes],
            dst_ref=gat.at[part, pl.ds(start, size), :, lanes],
            send_sem=ex_send.at[part, level],
            recv_sem=ex_recv.at[part, level],
            device_id=(me, 1 - core),
            device_id_type=MESH,
        )

    def add_gram(start, size, first):
        whole = gat.shape[3]
        half = whole // 2
        group = min(size, 8)
        if first:
            gram_ref[...] = jnp.zeros_like(gram_ref)

        def step(index, carry):
            part, piece = index // (size // group), index % (size // group)
            rows = gat[part, pl.ds(start + piece * group, group)].reshape(group * sub, whole)
            dims = (((0,), (0,)), ((), ()))
            gram_ref[0:half, :] += lax.dot_general(
                rows[:, :half], rows, dims, precision=HIGHEST, preferred_element_type=jnp.float32
            )
            gram_ref[half:, half:] += lax.dot_general(
                rows[:, half:], rows[:, half:], dims, precision=HIGHEST, preferred_element_type=jnp.float32
            )
            return carry

        lax.fori_loop(0, parts * (size // group), step, 0)

    for part in range(parts):
        gather_copy(part, levels - 1).start()
        core_copy(part, levels).start()
    for level in range(levels - 1, 0, -1):
        for part in range(parts):
            gather_copy(part, level).wait_recv()
            gather_copy(part, level - 1).start()
            core_copy(part, level).start()
    for level in range(levels, 0, -1):
        for part in range(parts):
            core_copy(part, level).wait_recv()
    add_gram(0, n // 2, True)
    for part in range(parts):
        gather_copy(part, 0).wait_recv()
        core_copy(part, 0).start()
    for part in range(parts):
        core_copy(part, 0).wait_recv()
    add_gram(n // 2, n // 2, False)
    for part in range(parts):
        for level in range(levels):
            reduce_copy(part, level).wait_send()
            gather_copy(part, level).wait_send()
        for level in range(levels + 1):
            core_copy(part, level).wait_send()


def exchange(outgoing, n, cores):
    count, width = outgoing.shape
    per = count // n
    levels = n.bit_length() - 1
    parts = 2
    orders = []
    for part in range(parts):
        order = list(range(levels))
        if part % 2 and levels > 1:
            order[0], order[1] = order[1], order[0]
        orders.append(tuple(order))
    slots = (parts, n, per // parts, width)
    sems = pltpu.SemaphoreType.DMA((parts, levels))
    whole = width * cores
    return pl.pallas_call(
        functools.partial(exchange_kernel, n, tuple(orders)),
        out_shape=(
            jax.ShapeDtypeStruct((per, width), jnp.float32),
            jax.ShapeDtypeStruct((whole, whole), jnp.float32),
        ),
        in_specs=[pl.BlockSpec(memory_space=pltpu.VMEM)],
        out_specs=(pl.BlockSpec(memory_space=pltpu.VMEM),) * 2,
        scratch_shapes=[
            pltpu.VMEM(slots, jnp.float32),
            pltpu.VMEM(slots, jnp.float32),
            pltpu.VMEM((parts, n, per // parts, whole), jnp.float32),
            sems, sems, sems, sems,
            pltpu.SemaphoreType.DMA((parts, levels + 1)),
            pltpu.SemaphoreType.DMA((parts, levels + 1)),
        ],
        compiler_params=pltpu.CompilerParams(
            collective_id=0, has_side_effects=True, vmem_limit_bytes=60 * 1024 * 1024
        ),
    )(outgoing.reshape(n, per, width))


def factor_block(block, inverse):
    size = block.shape[0]
    sub = lax.broadcasted_iota(jnp.int32, (8, size), 0)
    rest_a = block
    rest_b = None
    if inverse:
        rest_b = (
            lax.broadcasted_iota(jnp.int32, (size, size), 0) == lax.broadcasted_iota(jnp.int32, (size, size), 1)
        ).astype(jnp.float32)
    upper, lower = [], []
    for group in range(size // 8):
        first = group * 8
        columns = [jnp.broadcast_to(rest_a[:, first + j : first + j + 1], rest_a.shape) for j in range(8)]
        top_c, rest_c = [c[:8] for c in columns], [c[8:] for c in columns]
        more = first + 8 < size
        top_a, rest_a = rest_a[:8], rest_a[8:]
        if inverse:
            top_b, rest_b = rest_b[:8], rest_b[8:]
        for j in range(8):
            root = lax.rsqrt(top_c[j][j : j + 1])
            top_s = jnp.where(sub > j, top_c[j] * root, 0.0)
            row_a = top_a[j : j + 1] * root
            top_a = jnp.where(sub == j, row_a, top_a - top_s * row_a)
            if more:
                rest_s = rest_c[j] * root
                rest_a = rest_a - rest_s * row_a
            if inverse:
                row_b = top_b[j : j + 1] * root
                top_b = jnp.where(sub == j, row_b, top_b - top_s * row_b)
                if more:
                    rest_b = rest_b - rest_s * row_b
            for later in range(j + 1, 8):
                weight = top_c[later][j : j + 1] * root
                top_c[later] = top_c[later] - top_s * weight
                if more:
                    rest_c[later] = rest_c[later] - rest_s * weight
        upper.append(top_a)
        if inverse:
            lower.append(top_b)
    return jnp.concatenate(upper, axis=0), (jnp.concatenate(lower, axis=0) if inverse else None)


def cholesky_kernel(scale, gram_ref, out_ref, work, upper):
    size = gram_ref.shape[0]
    block = LANES
    work[...] = gram_ref[...] * scale
    upper[...] = jnp.zeros_like(upper)
    triangle = lax.broadcasted_iota(jnp.int32, (block, block), 0) <= lax.broadcasted_iota(
        jnp.int32, (block, block), 1
    )
    dims = (((0,), (0,)), ((), ()))
    for start in range(0, size, block):
        stop = start + block
        last = stop == size
        diagonal, inverse = factor_block(work[start:stop, start:stop], not last)
        upper[start:stop, start:stop] = jnp.where(triangle, diagonal, 0.0)
        if not last:
            panel = jnp.dot(
                inverse, work[start:stop, stop:], precision=HIGHEST, preferred_element_type=jnp.float32
            )
            upper[start:stop, stop:] = panel
            for row in range(stop, size, block):
                work[row : row + block, row:] -= lax.dot_general(
                    panel[:, row - stop : row - stop + block],
                    panel[:, row - stop :],
                    dims,
                    precision=HIGHEST,
                    preferred_element_type=jnp.float32,
                )
    width = out_ref.shape[1]
    out_ref[...] = upper[:, pl.ds(pl.multiple_of(lax.axis_index("cols") * width, width), width)]


def cholesky(gram, scale, width):
    size = gram.shape[0]
    return pl.pallas_call(
        functools.partial(cholesky_kernel, scale),
        out_shape=jax.ShapeDtypeStruct((size, width), jnp.float32),
        in_specs=[pl.BlockSpec(memory_space=pltpu.VMEM)],
        out_specs=pl.BlockSpec(memory_space=pltpu.VMEM),
        scratch_shapes=[pltpu.VMEM((size, size), jnp.float32)] * 2,
    )(gram)


def solution(mesh):
    n, cores = mesh.shape["rows"], mesh.shape["cols"]

    def body(design, signs, kept):
        widths = design.shape[1]
        outgoing = transform(design, signs, kept, design.shape[0] * n)
        sketch, gram = exchange(outgoing, n, cores)
        return (sketch, cholesky(gram, 1.0 / kept.shape[0], widths))

    return jax.shard_map(
        body,
        mesh=mesh,
        in_specs=(P("rows", "cols"), P("rows"), P()),
        out_specs=(P("rows", "cols"), P(None, "cols")),
        check_vma=False,
    )
```
